32 devices in a mesh: rep: 16 (over z, y, x), dom: 2 (over core).
Axes of the slice: x: 2, y: 2, z: 4, core: 2. Of those that a mesh axis runs over, the one named last changes fastest.
Arguments:
- protein_pos: float32 [3, 65536], P(None, ('rep', 'dom')), parts along dimension 1, may hold values from -4 to 4, as said below
- protein_vel: float32 [3, 65536], P(None, ('rep', 'dom')), parts along dimension 1, may hold values from -3 to 3
- inv_mass: float32 [65536], P(('rep', 'dom')), parts along dimension 0, may hold values from 0.0625 to 1
- bond_atoms: int32 [2, 40960], P(None, ('rep', 'dom')), parts along dimension 1, may hold values from 0 to 2047, as said below
- left_atoms: int32 [12288], P(('rep', 'dom')), parts along dimension 0, may hold values from 0 to 2047, as said below
- right_atoms: int32 [12288], P(('rep', 'dom')), parts along dimension 0, may hold values from 0 to 2047, as said below
- water_pos: float32 [9, 32768], P(None, ('rep', 'dom')), parts along dimension 1, may hold values from -3.2 to 3.2, as said below
- water_vel: float32 [9, 32768], P(None, ('rep', 'dom')), parts along dimension 1, may hold values from -3 to 3
Outputs:
- protein_velocity: float32 [3, 65536], P(None, ('rep', 'dom')), parts along dimension 1
- water_velocity: float32 [9, 32768], P(None, ('rep', 'dom')), parts along dimension 1
The draws below stay inside these ranges and needn't reach their ends.
There are 16 independent parts, one for each index of `rep`. The reference program is written for one: setup_inputs(seed, part) draws one part's arguments, and reference() takes and returns one part's arrays. A program takes and returns all parts, laid end to end along the dimension named above; each array names one. Nothing has to cross between parts.
Inputs may be any that keep to these rules, and one draw needn't show every extreme that they name: `bond_atoms`: indices within the domain's block of 2048 atoms; each column joins two different atoms; together with the cross bonds the bonds form a forest. `left_atoms`: distinct indices within the domain's block, none of them in right_atoms. `right_atoms`: distinct indices within the domain's block. `protein_pos`: every bond and every cross bond joins atoms 0.1 to 0.15 apart. `water_pos`: each column holds one rigid water: oxygen, then two hydrogens, 0.09572 from the oxygen and 0.15139 from each other.
All inputs are finite; a program needn't handle non-finite values.
Results may differ from the reference program's by a relative error of at most 0.0003.
Values sent between devices are 32-bit elements; how exact they have to be, the bound alone decides.
A program may use at most 64 MiB of HBM per device.

```python
import math
import jax
import jax.numpy as jnp
from jax import lax

PROT_DEV = 2048
HALO = 384
ORDER = 4
ITER = 2
BOND_DEV = 1280
PROTEIN = 4096
BONDS = 2560
CROSS = 768
WATERS = 2048
N_DOM = 2


oxygen_hydrogen = 0.09572


hydrogen_pair = 0.15139


def topology(key):
    base = jax.random.fold_in(key, 7)
    perms = jax.vmap(lambda single: jax.random.permutation(single, PROT_DEV))(jax.random.split(base, N_DOM)).astype(jnp.int32)
    mains = BOND_DEV - HALO
    nodes = jnp.arange(mains + 1, dtype=jnp.int32)
    parents = jnp.broadcast_to(jnp.maximum(nodes - 1, 0) // 3, (N_DOM, mains + 1)).astype(jnp.int32)
    return (perms, parents)


def draw_bond_atoms(key, part):
    perms, parents = topology(key)
    mains = BOND_DEV - HALO
    nodes = jnp.arange(1, mains + 1, dtype=jnp.int32)
    child_main = perms[:, HALO + 1:HALO + 1 + mains]
    parent_main = jnp.take_along_axis(perms, parents[:, nodes] + HALO, axis=1)
    child_cap = perms[:, HALO + mains + 1:HALO + mains + 1 + HALO]
    parent_cap = perms[:, :HALO]
    child = jnp.concatenate([child_main, child_cap], axis=1)
    parent = jnp.concatenate([parent_main, parent_cap], axis=1)
    return jnp.stack([child, parent]).reshape(2, N_DOM * BOND_DEV).astype(jnp.int32)


def draw_left_atoms(key, part):
    perms, parents = topology(key)
    return perms[:, :HALO].reshape(N_DOM * HALO).astype(jnp.int32)


def draw_right_atoms(key, part):
    perms, parents = topology(key)
    mains = BOND_DEV - HALO
    return perms[:, mains + 1:mains + 1 + HALO].reshape(N_DOM * HALO).astype(jnp.int32)


def bond_lengths(key, shape):
    return jnp.exp(jax.random.uniform(key, shape, jnp.float32, math.log(0.1), math.log(0.15)))


def random_steps(key, shape):
    keys = jax.random.split(key, 3)
    cosine = jax.random.uniform(keys[0], shape, jnp.float32, -1.0, 1.0)
    angle = jax.random.uniform(keys[1], shape, jnp.float32, 0.0, 2.0 * math.pi)
    sine = jnp.sqrt(jnp.maximum(1.0 - cosine * cosine, 0.0))
    lengths = bond_lengths(keys[2], shape)
    return jnp.stack([sine * jnp.cos(angle), sine * jnp.sin(angle), cosine], axis=1) * lengths[:, None, :]


def tetra_steps(key, index, sign):
    keys = jax.random.split(key, 2)
    table = jnp.array([[1.0, 1.0, 1.0], [1.0, -1.0, -1.0], [-1.0, 1.0, -1.0], [-1.0, -1.0, 1.0]], jnp.float32) / math.sqrt(3.0)
    pick = (index[..., None] == jnp.arange(4, dtype=jnp.int32)).astype(jnp.float32)
    direction = jnp.einsum('dnk,kc->dcn', pick, table) * sign[:, None, :]
    jitter = jnp.clip(jax.random.normal(keys[0], direction.shape, jnp.float32), -2.0, 2.0)
    direction = direction + 0.15 * jitter
    direction = direction / jnp.sqrt(jnp.sum(direction * direction, axis=1, keepdims=True))
    return direction * bond_lengths(keys[1], index.shape)[:, None, :]


def draw_protein_pos(key, part):
    perms, parents = topology(key)
    keys = jax.random.split(jax.random.fold_in(key, 21), 9)
    mains = BOND_DEV - HALO
    nodes = jnp.arange(mains + 1, dtype=jnp.int32)
    turns = jax.random.randint(keys[5], (N_DOM, mains + 1), 0, 3, dtype=jnp.int32)
    first_dir = jax.random.randint(keys[6], (N_DOM, 1), 0, 4, dtype=jnp.int32)
    slot = jnp.maximum(nodes - 1, 0) % 3
    index = jnp.broadcast_to(first_dir, (N_DOM, mains + 1)).astype(jnp.int32)
    depth = jnp.zeros((N_DOM, mains + 1), jnp.int32)
    for rounds in range(16):
        up_index = jnp.take_along_axis(index, parents, axis=1)
        up_turn = jnp.take_along_axis(turns, parents, axis=1)
        up_depth = jnp.take_along_axis(depth, parents, axis=1)
        index = jnp.where(nodes == 0, first_dir, (up_index + 1 + (slot + up_turn) % 3) % 4).astype(jnp.int32)
        depth = jnp.where(nodes == 0, 0, up_depth + 1).astype(jnp.int32)
    sign = jnp.where(depth % 2 == 1, 1.0, -1.0).astype(jnp.float32)
    steps = tetra_steps(keys[0], index, sign)
    steps = steps.at[:, :, 0].set(0.0)
    root = jax.random.uniform(keys[1], (N_DOM, 3), jnp.float32, -1.0, 1.0)
    total = steps
    pointer = parents
    for rounds in range(6):
        total = total + jnp.take_along_axis(total, jnp.broadcast_to(pointer[:, None, :], total.shape), axis=2)
        pointer = jnp.take_along_axis(pointer, pointer, axis=1)
    main_pos = total + root[:, :, None]
    anchor_pos = main_pos[:, :, mains + 1 - HALO:mains + 1]
    anchor_index = jnp.roll(index[:, mains + 1 - HALO:mains + 1], 1, axis=0)
    anchor_depth = jnp.roll(depth[:, mains + 1 - HALO:mains + 1], 1, axis=0)
    anchor_sign = jnp.where(anchor_depth % 2 == 0, 1.0, -1.0).astype(jnp.float32)
    cap_index = (anchor_index + 1 + jax.random.randint(keys[7], (N_DOM, HALO), 0, 3, dtype=jnp.int32)) % 4
    child_index = (cap_index + 1 + jax.random.randint(keys[8], (N_DOM, HALO), 0, 3, dtype=jnp.int32)) % 4
    cap_pos = jnp.roll(anchor_pos, 1, axis=0) + tetra_steps(keys[2], cap_index, anchor_sign)
    child_pos = cap_pos + tetra_steps(keys[3], child_index, -anchor_sign)
    lone_pos = root[:, :, None] + random_steps(keys[4], (N_DOM, HALO - 1))

    def place(perm, main_part, cap_part, child_part, lone_part):
        field = jnp.zeros((3, PROT_DEV), jnp.float32)
        field = field.at[:, perm[HALO:HALO + mains + 1]].set(main_part)
        field = field.at[:, perm[:HALO]].set(cap_part)
        field = field.at[:, perm[HALO + mains + 1:HALO + mains + 1 + HALO]].set(child_part)
        return field.at[:, perm[PROT_DEV - HALO + 1:]].set(lone_part)
    placed = jax.vmap(place)(perms, main_pos, cap_pos, child_pos, lone_pos)
    return jnp.transpose(placed, (1, 0, 2)).reshape(3, N_DOM * PROT_DEV)


def draw_water_pos(key, part):
    keys = jax.random.split(jax.random.fold_in(key, 31), 4)
    oxygen = jax.random.uniform(keys[0], (3, WATERS), jnp.float32, -3.0, 3.0)
    first_angle = jax.random.uniform(keys[1], (WATERS,), jnp.float32, -math.pi, math.pi)
    second_angle = jax.random.uniform(keys[2], (WATERS,), jnp.float32, -math.pi, math.pi)
    third_angle = jax.random.uniform(keys[3], (WATERS,), jnp.float32, -math.pi, math.pi)
    cos_a, sin_a = (jnp.cos(first_angle), jnp.sin(first_angle))
    cos_b, sin_b = (jnp.cos(second_angle), jnp.sin(second_angle))
    cos_c, sin_c = (jnp.cos(third_angle), jnp.sin(third_angle))
    column_one = jnp.stack([cos_a * cos_c - sin_a * cos_b * sin_c, sin_a * cos_c + cos_a * cos_b * sin_c, sin_b * sin_c])
    column_two = jnp.stack([-cos_a * sin_c - sin_a * cos_b * cos_c, -sin_a * sin_c + cos_a * cos_b * cos_c, sin_b * cos_c])
    half = 0.5 * hydrogen_pair
    height = math.sqrt(oxygen_hydrogen * oxygen_hydrogen - half * half)
    first = oxygen + half * column_one - height * column_two
    second = oxygen - half * column_one - height * column_two
    return jnp.concatenate([oxygen, first, second], axis=0)


def block_levels(own_key, shape, shards, least, high):
    gain = 1.0
    for axis_at, shards_of in shards:
        draws = jax.random.uniform(jax.random.fold_in(jax.random.fold_in(own_key, 6), axis_at), (shards_of,), jnp.float32, least / len(shards), high / len(shards))
        gain = gain * jnp.repeat(jnp.exp(draws), shape[axis_at] // shards_of).reshape((-1,) + (1,) * (len(shape) - 1 - axis_at))
    return gain


def gaussian(key, dims, spread, bound, cuts=(), kind=jnp.bfloat16):
    level = block_levels(key, dims, cuts, -0.22, 0.18) if cuts else 1.0
    entries = jax.random.normal(key, dims, jnp.float32) * spread * level
    return jnp.minimum(jnp.maximum(entries, -bound), bound).astype(kind)


def setup_inputs(seed: int = 0, part: int = 0) -> dict:
    seeds = jax.random.split(jax.random.key(seed), 9)
    part_splits = jax.random.split(jax.random.fold_in(seeds[8], part), 9)
    return {
        "protein_pos": draw_protein_pos(jax.random.fold_in(jax.random.fold_in(seeds[8], part), 71), part),
        "protein_vel": gaussian(part_splits[1], (3, PROTEIN), 1.0, 3.0, ((1, 2),), jnp.float32),
        "inv_mass": jnp.clip(jnp.exp(math.log(1.0) - 2.7725887 * jax.random.uniform(part_splits[2], (PROTEIN,), jnp.float32) ** block_levels(part_splits[2], (PROTEIN,), ((0, 2),), -0.2, 0.2)), 0.0625, 1.0),
        "bond_atoms": draw_bond_atoms(jax.random.fold_in(jax.random.fold_in(seeds[8], part), 71), part),
        "left_atoms": draw_left_atoms(jax.random.fold_in(jax.random.fold_in(seeds[8], part), 71), part),
        "right_atoms": draw_right_atoms(jax.random.fold_in(jax.random.fold_in(seeds[8], part), 71), part),
        "water_pos": draw_water_pos(jax.random.fold_in(jax.random.fold_in(seeds[8], part), 71), part),
        "water_vel": gaussian(part_splits[7], (9, WATERS), 1.0, 3.0, ((1, 2),), jnp.float32),
    }


time_step = 0.002
mass_oxygen = 15.9994
mass_hydrogen = 1.008
oxygen_hydrogen = 0.09572
hydrogen_pair = 0.15139
total_mass = mass_oxygen + 2.0 * mass_hydrogen
half_pair = 0.5 * hydrogen_pair
water_height = math.sqrt(oxygen_hydrogen * oxygen_hydrogen - half_pair * half_pair)
oxygen_reach = 2.0 * mass_hydrogen * water_height / total_mass
hydrogen_reach = water_height - oxygen_reach

def cross_product(left, right):
    return jnp.stack([left[1] * right[2] - left[2] * right[1], left[2] * right[0] - left[0] * right[2], left[0] * right[1] - left[1] * right[0]])

def inner(left, right):
    return lax.optimization_barrier(jnp.sum(left * right, axis=0))

def settle(before, after):
    old_oxygen, old_first, old_second = (before[0:3], before[3:6], before[6:9])
    new_oxygen, new_first, new_second = (after[0:3], after[3:6], after[6:9])
    center = (mass_oxygen * new_oxygen + mass_hydrogen * (new_first + new_second)) / total_mass
    old_b = old_first - old_oxygen
    old_c = old_second - old_oxygen
    rel_a = new_oxygen - center
    rel_b = new_first - center
    rel_c = new_second - center
    normal = cross_product(old_b, old_c)
    side = cross_product(rel_a, normal)
    upward = cross_product(normal, side)
    axis_z = normal / jnp.sqrt(inner(normal, normal))
    axis_x = side / jnp.sqrt(inner(side, side))
    axis_y = upward / jnp.sqrt(inner(upward, upward))
    oldb_x = inner(axis_x, old_b)
    oldb_y = inner(axis_y, old_b)
    oldc_x = inner(axis_x, old_c)
    oldc_y = inner(axis_y, old_c)
    newa_z = inner(axis_z, rel_a)
    newb_x = inner(axis_x, rel_b)
    newb_y = inner(axis_y, rel_b)
    newb_z = inner(axis_z, rel_b)
    newc_x = inner(axis_x, rel_c)
    newc_y = inner(axis_y, rel_c)
    newc_z = inner(axis_z, rel_c)
    sin_phi = newa_z / oxygen_reach
    cos_phi = jnp.sqrt(1.0 - sin_phi * sin_phi)
    sin_psi = (newb_z - newc_z) / (2.0 * half_pair * cos_phi)
    cos_psi = jnp.sqrt(1.0 - sin_psi * sin_psi)
    rest_ay = oxygen_reach * cos_phi
    rest_bx = -half_pair * cos_psi
    lowered = -hydrogen_reach * cos_phi
    tilted = half_pair * sin_psi * sin_phi
    rest_by = lowered - tilted
    rest_cy = lowered + tilted
    alpha = rest_bx * (oldb_x - oldc_x) + oldb_y * rest_by + oldc_y * rest_cy
    beta = rest_bx * (oldc_y - oldb_y) + oldb_x * rest_by + oldc_x * rest_cy
    gamma = oldb_x * newb_y - newb_x * oldb_y + oldc_x * newc_y - newc_x * oldc_y
    summed = alpha * alpha + beta * beta
    sin_theta = (alpha * gamma - beta * jnp.sqrt(summed - gamma * gamma)) / summed
    cos_theta = jnp.sqrt(1.0 - sin_theta * sin_theta)
    final_ax = -rest_ay * sin_theta
    final_ay = rest_ay * cos_theta
    final_bx = rest_bx * cos_theta - rest_by * sin_theta
    final_by = rest_bx * sin_theta + rest_by * cos_theta
    final_cx = -rest_bx * cos_theta - rest_cy * sin_theta
    final_cy = -rest_bx * sin_theta + rest_cy * cos_theta
    oxygen = center + axis_x * final_ax + axis_y * final_ay + axis_z * newa_z
    first = center + axis_x * final_bx + axis_y * final_by + axis_z * newb_z
    second = center + axis_x * final_cx + axis_y * final_cy + axis_z * newc_z
    return jnp.concatenate([oxygen, first, second], axis=0)

def reference(protein_pos, protein_vel, inv_mass, bond_atoms, left_atoms, right_atoms, water_pos, water_vel):
    bond_domain = jnp.arange(BONDS, dtype=jnp.int32) // BOND_DEV
    slot_domain = jnp.arange(CROSS, dtype=jnp.int32) // HALO
    next_domain = (slot_domain + 1) % N_DOM
    anchors = right_atoms + slot_domain * PROT_DEV
    capped = jnp.roll(left_atoms, -HALO) + next_domain * PROT_DEV
    first = jnp.concatenate([bond_atoms[0] + bond_domain * PROT_DEV, anchors]).astype(jnp.int32)
    second = jnp.concatenate([bond_atoms[1] + bond_domain * PROT_DEV, capped]).astype(jnp.int32)
    moved = protein_pos + time_step * protein_vel
    diff = protein_pos[:, first] - protein_pos[:, second]
    length = jnp.sqrt(inner(diff, diff))
    unit = diff / length
    scale = 1.0 / jnp.sqrt(inv_mass[first] + inv_mass[second])

    def atom_field(values):
        weighted = unit * (scale * values)
        force = jnp.zeros((3, PROTEIN), jnp.float32).at[:, first].add(weighted).at[:, second].add(-weighted)
        return inv_mass * force

    def expand(rhs):
        total = rhs
        current = rhs
        for order_index in range(ORDER):
            field = atom_field(current)
            current = current - scale * inner(unit, field[:, first] - field[:, second])
            total = total + current
        return total
    rhs = scale * (inner(unit, moved[:, first] - moved[:, second]) - length)
    delta = -atom_field(expand(rhs))
    for round_index in range(ITER):
        now = moved + delta
        gap = now[:, first] - now[:, second]
        target = jnp.sqrt(2.0 * length * length - inner(gap, gap))
        rhs = scale * (length - target)
        delta = delta - atom_field(expand(rhs))
    protein_velocity = protein_vel + delta / time_step
    water_moved = water_pos + time_step * water_vel
    settled = settle(water_pos, water_moved)
    water_velocity = water_vel + (settled - water_moved) / time_step
    return (protein_velocity, water_velocity)
```

```python
import functools
import math

import jax
import jax.numpy as jnp
from jax import lax
from jax.experimental import pallas as pl
from jax.experimental.pallas import tpu as pltpu
from jax.sharding import PartitionSpec as P

ORDER = 4
ITER = 2
LANES = 128
SUB = 8


time_step = 0.002
mass_oxygen = 15.9994
mass_hydrogen = 1.008
oxygen_hydrogen = 0.09572
hydrogen_pair = 0.15139
total_mass = mass_oxygen + 2.0 * mass_hydrogen
half_pair = 0.5 * hydrogen_pair
water_height = math.sqrt(oxygen_hydrogen * oxygen_hydrogen - half_pair * half_pair)
oxygen_reach = 2.0 * mass_hydrogen * water_height / total_mass
hydrogen_reach = water_height - oxygen_reach


def cross_product(left, right):
    return [
        left[1] * right[2] - left[2] * right[1],
        left[2] * right[0] - left[0] * right[2],
        left[0] * right[1] - left[1] * right[0],
    ]


def inner(left, right):
    return left[0] * right[0] + left[1] * right[1] + left[2] * right[2]


def minus(left, right):
    return [a - b for a, b in zip(left, right)]


def settle(before, after):
    old_oxygen, old_first, old_second = (before[0:3], before[3:6], before[6:9])
    new_oxygen, new_first, new_second = (after[0:3], after[3:6], after[6:9])
    center = [
        (mass_oxygen * o + mass_hydrogen * (f + s)) / total_mass
        for o, f, s in zip(new_oxygen, new_first, new_second)
    ]
    old_b = minus(old_first, old_oxygen)
    old_c = minus(old_second, old_oxygen)
    rel_a = minus(new_oxygen, center)
    rel_b = minus(new_first, center)
    rel_c = minus(new_second, center)
    normal = cross_product(old_b, old_c)
    side = cross_product(rel_a, normal)
    upward = cross_product(normal, side)

    def normed(vector):
        size = jnp.sqrt(inner(vector, vector))
        return [a / size for a in vector]

    axis_z = normed(normal)
    axis_x = normed(side)
    axis_y = normed(upward)
    oldb_x = inner(axis_x, old_b)
    oldb_y = inner(axis_y, old_b)
    oldc_x = inner(axis_x, old_c)
    oldc_y = inner(axis_y, old_c)
    newa_z = inner(axis_z, rel_a)
    newb_x = inner(axis_x, rel_b)
    newb_y = inner(axis_y, rel_b)
    newb_z = inner(axis_z, rel_b)
    newc_x = inner(axis_x, rel_c)
    newc_y = inner(axis_y, rel_c)
    newc_z = inner(axis_z, rel_c)
    sin_phi = newa_z / oxygen_reach
    cos_phi = jnp.sqrt(1.0 - sin_phi * sin_phi)
    sin_psi = (newb_z - newc_z) / (2.0 * half_pair * cos_phi)
    cos_psi = jnp.sqrt(1.0 - sin_psi * sin_psi)
    rest_ay = oxygen_reach * cos_phi
    rest_bx = -half_pair * cos_psi
    lowered = -hydrogen_reach * cos_phi
    tilted = half_pair * sin_psi * sin_phi
    rest_by = lowered - tilted
    rest_cy = lowered + tilted
    alpha = rest_bx * (oldb_x - oldc_x) + oldb_y * rest_by + oldc_y * rest_cy
    beta = rest_bx * (oldc_y - oldb_y) + oldb_x * rest_by + oldc_x * rest_cy
    gamma = oldb_x * newb_y - newb_x * oldb_y + oldc_x * newc_y - newc_x * oldc_y
    summed = alpha * alpha + beta * beta
    sin_theta = (alpha * gamma - beta * jnp.sqrt(summed - gamma * gamma)) / summed
    cos_theta = jnp.sqrt(1.0 - sin_theta * sin_theta)
    final_ax = -rest_ay * sin_theta
    final_ay = rest_ay * cos_theta
    final_bx = rest_bx * cos_theta - rest_by * sin_theta
    final_by = rest_bx * sin_theta + rest_by * cos_theta
    final_cx = -rest_bx * cos_theta - rest_cy * sin_theta
    final_cy = -rest_bx * sin_theta + rest_cy * cos_theta

    def placed(x, y, z):
        return [
            center[c] + axis_x[c] * x + axis_y[c] * y + axis_z[c] * z for c in range(3)
        ]

    return (
        placed(final_ax, final_ay, newa_z)
        + placed(final_bx, final_by, newb_z)
        + placed(final_cx, final_cy, newc_z)
    )


def lane_gather(table, index):
    return jnp.take_along_axis(table, index, axis=1, mode="promise_in_bounds")


def kernel(
    n, axis, pos, vel, mass, bonds, left, right, wpos, wvel, out_p, out_w,
    pos_x, vel_x, mass_x, bonds_x, left_x, right_x,
    first_s, second_s, packed_s, rows_s, lanes_s, lhs_s, field_s, water_s,
    send_sem, recv_sem,
):
    atom_rows = mass.shape[0]
    bond_rows = bonds.shape[1] // LANES
    halo_rows = left.shape[0]
    used = bond_rows + halo_rows
    con_rows = first_s.shape[1]
    tiles = con_rows // SUB
    half_rows = 2 * used
    water_rows = wpos.shape[1] // LANES

    own = (pos, vel, mass, bonds, left, right)
    others = (pos_x, vel_x, mass_x, bonds_x, left_x, right_x)
    me = lax.axis_index(axis)
    copies = []
    if n > 1:
        barrier = pltpu.get_barrier_semaphore()
        for k in range(1, n):
            peer = lax.rem(me + k, n)
            pl.semaphore_signal(
                barrier, inc=1, device_id={axis: peer},
                device_id_type=pl.DeviceIdType.MESH,
            )
        pl.semaphore_wait(barrier, n - 1)
        for k in range(1, n):
            peer = lax.rem(me + n - k, n)
            for t in range(len(own)):
                copy = pltpu.make_async_remote_copy(
                    src_ref=own[t],
                    dst_ref=others[t].at[k - 1],
                    send_sem=send_sem.at[k - 1, t],
                    recv_sem=recv_sem.at[k - 1, t],
                    device_id={axis: peer},
                    device_id_type=pl.DeviceIdType.MESH,
                )
                copy.start()
                copies.append(copy)

    components = wpos.shape[0]
    for source, base in ((wpos, 0), (wvel, components)):
        for c in range(components):
            for r in range(water_rows):
                water_s[base + c, pl.ds(r, 1), :] = source[
                    pl.ds(c, 1), pl.ds(r * LANES, LANES)
                ]
    before = [water_s[c] for c in range(components)]
    speed = [water_s[components + c] for c in range(components)]
    after = [b + time_step * v for b, v in zip(before, speed)]
    settled = settle(before, after)
    for c in range(components):
        water_s[c] = speed[c] + (settled[c] - after[c]) / time_step
    for c in range(components):
        for r in range(water_rows):
            out_w[pl.ds(c, 1), pl.ds(r * LANES, LANES)] = water_s[c, pl.ds(r, 1), :]

    for copy in copies:
        copy.wait()

    def data(k):
        return own if k == 0 else tuple(ref.at[k - 1] for ref in others)

    for k in range(n):
        bonds_k, right_k = data(k)[3], data(k)[5]
        left_k = data((k + 1) % n)[4]
        first_s[k, pl.ds(used, con_rows - used), :] = jnp.zeros(
            (con_rows - used, LANES), jnp.int32
        )
        second_s[k, pl.ds(used, con_rows - used), :] = jnp.zeros(
            (con_rows - used, LANES), jnp.int32
        )
        for r in range(bond_rows):
            first_s[k, pl.ds(r, 1), :] = bonds_k[pl.ds(0, 1), pl.ds(r * LANES, LANES)]
            second_s[k, pl.ds(r, 1), :] = bonds_k[pl.ds(1, 1), pl.ds(r * LANES, LANES)]
        first_s[k, pl.ds(bond_rows, halo_rows), :] = right_k[...]
        second_s[k, pl.ds(bond_rows, halo_rows), :] = left_k[...]

    row_iota = lax.broadcasted_iota(jnp.int32, (atom_rows, LANES), 0)
    lane_iota = lax.broadcasted_iota(jnp.int32, (LANES, LANES), 0)
    half_source = []
    for k in range(n):
        sources = [(k, r, first_s, k, 1.0) for r in range(used)]
        sources += [(k, r, second_s, k, -1.0) for r in range(bond_rows)]
        back = (k + n - 1) % n
        sources += [(back, r, second_s, back, -1.0) for r in range(bond_rows, used)]
        half_source.append([(s[0], s[1]) for s in sources])
        for p, (_, r, ref, slot, sign) in enumerate(sources):
            index = ref[slot, pl.ds(r, 1), :]
            rows_s[k, p] = jnp.where(row_iota == (index >> 7), sign, 0.0).astype(
                jnp.bfloat16
            )
            lanes_s[k, :, pl.ds(p * LANES, LANES)] = jnp.where(
                lane_iota == (index & 127), 1.0, 0.0
            ).astype(jnp.bfloat16)

    position = lax.broadcasted_iota(jnp.int32, (SUB, LANES), 0)
    valid = [position + v * SUB < used for v in range(tiles)]

    def gathered(k, tables):
        following = (k + 1) % n
        firsts = [[None] * tiles for _ in tables]
        seconds = [[None] * tiles for _ in tables]
        for v in range(tiles):
            index_i = first_s[k, pl.ds(v * SUB, SUB), :]
            index_j = second_s[k, pl.ds(v * SUB, SUB), :]
            lane_i, row_i = index_i & 127, index_i >> 7
            lane_j, row_j = index_j & 127, index_j >> 7
            low, high = v * SUB, (v + 1) * SUB
            for r in range(atom_rows):
                hit_i = row_i == r
                hit_j = row_j == r
                for c, table in enumerate(tables):
                    mine = jnp.broadcast_to(table(k, r), (SUB, LANES))
                    if high <= bond_rows:
                        there = mine
                    else:
                        there = jnp.broadcast_to(table(following, r), (SUB, LANES))
                        if low < bond_rows:
                            there = jnp.where(position + low < bond_rows, mine, there)
                    got_i = lane_gather(mine, lane_i)
                    got_j = lane_gather(there, lane_j)
                    if r > 0:
                        got_i = jnp.where(hit_i, got_i, firsts[c][v])
                        got_j = jnp.where(hit_j, got_j, seconds[c][v])
                    firsts[c][v] = got_i
                    seconds[c][v] = got_j
        join = lambda parts: jnp.concatenate(parts, axis=0)
        return [join(f) for f in firsts], [join(s) for s in seconds]

    valid = jnp.concatenate(valid, axis=0)
    unit, length, scale, gap, value = [], [], [], [], []
    for k in range(n):
        tables = []
        for which in (0, 1):
            for c in range(3):
                tables.append(
                    lambda slot, r, which=which, c=c: data(slot)[which][
                        pl.ds(c, 1), pl.ds(r * LANES, LANES)
                    ]
                )
        tables.append(lambda slot, r: data(slot)[2][pl.ds(r, 1), :])
        at_i, at_j = gathered(k, tables)
        diff = minus(at_i[0:3], at_j[0:3])
        size = jnp.where(valid, jnp.sqrt(inner(diff, diff)), 1.0)
        unit.append([d / size for d in diff])
        length.append(size)
        scale.append(jnp.where(valid, 1.0 / jnp.sqrt(at_i[6] + at_j[6]), 0.0))
        moved_i = [p + time_step * q for p, q in zip(at_i[0:3], at_i[3:6])]
        moved_j = [p + time_step * q for p, q in zip(at_j[0:3], at_j[3:6])]
        gap.append(minus(moved_i, moved_j))
        value.append(scale[k] * (inner(unit[k], gap[k]) - length[k]))
    scaled_unit = [[scale[k] * u for u in unit[k]] for k in range(n)]

    def make_field(values, slots):
        for k in range(n):
            for c in range(3):
                weighted = scaled_unit[k][c] * values[k]
                high = weighted.astype(jnp.bfloat16).astype(jnp.float32)
                packed_s[k, c] = high
                packed_s[k, 3 + c] = weighted - high
        for k in slots:
            for p, (slot, r) in enumerate(half_source[k]):
                hot = rows_s[k, p]
                for j in range(6):
                    wide = jnp.broadcast_to(
                        packed_s[slot, j, pl.ds(r, 1), :], (atom_rows, LANES)
                    ).astype(jnp.bfloat16)
                    lhs_s[k, pl.ds(j * atom_rows, atom_rows), pl.ds(p * LANES, LANES)] = (
                        wide * hot
                    )
            summed = lax.dot_general(
                lhs_s[k], lanes_s[k], (((1,), (1,)), ((), ())),
                preferred_element_type=jnp.float32,
            )
            weight = data(k)[2][...]
            for c in range(3):
                field_s[k, c] = weight * (
                    summed[c * atom_rows:(c + 1) * atom_rows]
                    + summed[(3 + c) * atom_rows:(4 + c) * atom_rows]
                )

    field_tables = [
        lambda slot, r, c=c: field_s[slot, c, pl.ds(r, 1), :] for c in range(3)
    ]

    def field_gap(k):
        at_i, at_j = gathered(k, field_tables)
        return minus(at_i, at_j)

    everyone = range(n)

    def one_order(_, carry):
        current, total = carry
        make_field(current, everyone)
        current = [
            current[k] - inner(scaled_unit[k], field_gap(k)) for k in everyone
        ]
        return current, [t + x for t, x in zip(total, current)]

    moved_by = None
    for round_index in range(ITER + 1):
        _, total = lax.fori_loop(0, ORDER, one_order, (value, value))
        last = round_index == ITER
        make_field(total, range(1) if last else everyone)
        own_field = [field_s[0, c] for c in range(3)]
        moved_by = (
            own_field if moved_by is None
            else [m + f for m, f in zip(moved_by, own_field)]
        )
        if not last:
            gap = [minus(gap[k], field_gap(k)) for k in everyone]
            value = []
            for k in everyone:
                target = jnp.sqrt(2.0 * length[k] * length[k] - inner(gap[k], gap[k]))
                value.append(scale[k] * (length[k] - target))
    for c in range(3):
        field_s[0, c] = moved_by[c] / time_step
    for c in range(3):
        for r in range(atom_rows):
            cols = pl.ds(r * LANES, LANES)
            out_p[pl.ds(c, 1), cols] = (
                vel[pl.ds(c, 1), cols] - field_s[0, c, pl.ds(r, 1), :]
            )


def on_device(
    n, protein_pos, protein_vel, inv_mass, bond_atoms, left_atoms, right_atoms, water_pos, water_vel
):
    atoms = protein_pos.shape[1]
    atom_rows = atoms // LANES
    bond_rows = bond_atoms.shape[1] // LANES
    halo_rows = left_atoms.shape[0] // LANES
    con_rows = -(-(bond_rows + halo_rows + 1) // SUB) * SUB
    half = 2 * (bond_rows + halo_rows)
    others = max(n - 1, 1)
    mass = inv_mass.reshape(atom_rows, LANES)
    left = left_atoms.reshape(halo_rows, LANES)
    right = right_atoms.reshape(halo_rows, LANES)
    operands = (protein_pos, protein_vel, mass, bond_atoms, left, right, water_pos, water_vel)
    vmem = pl.BlockSpec(memory_space=pltpu.VMEM)
    return pl.pallas_call(
        functools.partial(kernel, n, "dom"),
        out_shape=(
            jax.ShapeDtypeStruct(protein_vel.shape, jnp.float32),
            jax.ShapeDtypeStruct(water_vel.shape, jnp.float32),
        ),
        in_specs=[vmem] * len(operands),
        out_specs=(vmem, vmem),
        scratch_shapes=[
            pltpu.VMEM((others,) + x.shape, x.dtype) for x in operands[:6]
        ] + [
            pltpu.VMEM((n, con_rows, LANES), jnp.int32),
            pltpu.VMEM((n, con_rows, LANES), jnp.int32),
            pltpu.VMEM((n, 6, con_rows, LANES), jnp.float32),
            pltpu.VMEM((n, half, atom_rows, LANES), jnp.bfloat16),
            pltpu.VMEM((n, LANES, half * LANES), jnp.bfloat16),
            pltpu.VMEM((n, 6 * atom_rows, half * LANES), jnp.bfloat16),
            pltpu.VMEM((n, 3, atom_rows, LANES), jnp.float32),
            pltpu.VMEM((2 * water_pos.shape[0], water_pos.shape[1] // LANES, LANES), jnp.float32),
            pltpu.SemaphoreType.DMA((others, 6)),
            pltpu.SemaphoreType.DMA((others, 6)),
        ],
        compiler_params=pltpu.CompilerParams(
            collective_id=0, has_side_effects=True, vmem_limit_bytes=60 * 1024 * 1024
        ),
    )(*operands)


def solution(mesh):
    in_specs = (
        P(None, ("rep", "dom")),
        P(None, ("rep", "dom")),
        P(("rep", "dom")),
        P(None, ("rep", "dom")),
        P(("rep", "dom")),
        P(("rep", "dom")),
        P(None, ("rep", "dom")),
        P(None, ("rep", "dom")),
    )
    out_specs = (P(None, ("rep", "dom")), P(None, ("rep", "dom")))
    return jax.shard_map(
        functools.partial(on_device, mesh.shape["dom"]),
        mesh=mesh, in_specs=in_specs, out_specs=out_specs, check_vma=False,
    )
```

```python
import functools
import math

import jax
import jax.numpy as jnp
from jax import lax
from jax.experimental import pallas as pl
from jax.experimental.pallas import tpu as pltpu
from jax.sharding import PartitionSpec as P

ORDER = 4
ITER = 2
LANES = 128
SUB = 8


time_step = 0.002
mass_oxygen = 15.9994
mass_hydrogen = 1.008
oxygen_hydrogen = 0.09572
hydrogen_pair = 0.15139
total_mass = mass_oxygen + 2.0 * mass_hydrogen
half_pair = 0.5 * hydrogen_pair
water_height = math.sqrt(oxygen_hydrogen * oxygen_hydrogen - half_pair * half_pair)
oxygen_reach = 2.0 * mass_hydrogen * water_height / total_mass
hydrogen_reach = water_height - oxygen_reach


def cross_product(left, right):
    return [
        left[1] * right[2] - left[2] * right[1],
        left[2] * right[0] - left[0] * right[2],
        left[0] * right[1] - left[1] * right[0],
    ]


def inner(left, right):
    return left[0] * right[0] + left[1] * right[1] + left[2] * right[2]


def minus(left, right):
    return [a - b for a, b in zip(left, right)]


def settle(before, after):
    old_oxygen, old_first, old_second = (before[0:3], before[3:6], before[6:9])
    new_oxygen, new_first, new_second = (after[0:3], after[3:6], after[6:9])
    center = [
        (mass_oxygen * o + mass_hydrogen * (f + s)) / total_mass
        for o, f, s in zip(new_oxygen, new_first, new_second)
    ]
    old_b = minus(old_first, old_oxygen)
    old_c = minus(old_second, old_oxygen)
    rel_a = minus(new_oxygen, center)
    rel_b = minus(new_first, center)
    rel_c = minus(new_second, center)
    normal = cross_product(old_b, old_c)
    side = cross_product(rel_a, normal)
    upward = cross_product(normal, side)

    def normed(vector):
        size = jnp.sqrt(inner(vector, vector))
        return [a / size for a in vector]

    axis_z = normed(normal)
    axis_x = normed(side)
    axis_y = normed(upward)
    oldb_x = inner(axis_x, old_b)
    oldb_y = inner(axis_y, old_b)
    oldc_x = inner(axis_x, old_c)
    oldc_y = inner(axis_y, old_c)
    newa_z = inner(axis_z, rel_a)
    newb_x = inner(axis_x, rel_b)
    newb_y = inner(axis_y, rel_b)
    newb_z = inner(axis_z, rel_b)
    newc_x = inner(axis_x, rel_c)
    newc_y = inner(axis_y, rel_c)
    newc_z = inner(axis_z, rel_c)
    sin_phi = newa_z / oxygen_reach
    cos_phi = jnp.sqrt(1.0 - sin_phi * sin_phi)
    sin_psi = (newb_z - newc_z) / (2.0 * half_pair * cos_phi)
    cos_psi = jnp.sqrt(1.0 - sin_psi * sin_psi)
    rest_ay = oxygen_reach * cos_phi
    rest_bx = -half_pair * cos_psi
    lowered = -hydrogen_reach * cos_phi
    tilted = half_pair * sin_psi * sin_phi
    rest_by = lowered - tilted
    rest_cy = lowered + tilted
    alpha = rest_bx * (oldb_x - oldc_x) + oldb_y * rest_by + oldc_y * rest_cy
    beta = rest_bx * (oldc_y - oldb_y) + oldb_x * rest_by + oldc_x * rest_cy
    gamma = oldb_x * newb_y - newb_x * oldb_y + oldc_x * newc_y - newc_x * oldc_y
    summed = alpha * alpha + beta * beta
    sin_theta = (alpha * gamma - beta * jnp.sqrt(summed - gamma * gamma)) / summed
    cos_theta = jnp.sqrt(1.0 - sin_theta * sin_theta)
    final_ax = -rest_ay * sin_theta
    final_ay = rest_ay * cos_theta
    final_bx = rest_bx * cos_theta - rest_by * sin_theta
    final_by = rest_bx * sin_theta + rest_by * cos_theta
    final_cx = -rest_bx * cos_theta - rest_cy * sin_theta
    final_cy = -rest_bx * sin_theta + rest_cy * cos_theta

    def placed(x, y, z):
        return [
            center[c] + axis_x[c] * x + axis_y[c] * y + axis_z[c] * z for c in range(3)
        ]

    return (
        placed(final_ax, final_ay, newa_z)
        + placed(final_bx, final_by, newb_z)
        + placed(final_cx, final_cy, newc_z)
    )


def lane_gather(table, index):
    return jnp.take_along_axis(table, index, axis=1, mode="promise_in_bounds")


def kernel(
    n, axis, pos, vel, mass, bonds, left, right, wpos, wvel, out_p, out_w,
    pos_x, vel_x, mass_x, bonds_x, left_x, right_x,
    first_s, second_s, packed_s, rows_s, lanes_s, lhs_s, field_s, water_s,
    send_sem, recv_sem,
):
    atom_rows = mass.shape[0]
    bond_rows = bonds.shape[1] // LANES
    halo_rows = left.shape[0]
    used = bond_rows + halo_rows
    con_rows = first_s.shape[1]
    tiles = con_rows // SUB
    half_rows = 2 * used
    water_rows = wpos.shape[1] // LANES

    own = (pos, vel, mass, bonds, left, right)
    others = (pos_x, vel_x, mass_x, bonds_x, left_x, right_x)
    me = lax.axis_index(axis)
    copies = []
    if n > 1:
        barrier = pltpu.get_barrier_semaphore()
        for k in range(1, n):
            peer = lax.rem(me + k, n)
            pl.semaphore_signal(
                barrier, inc=1, device_id={axis: peer},
                device_id_type=pl.DeviceIdType.MESH,
            )
        pl.semaphore_wait(barrier, n - 1)
        for k in range(1, n):
            peer = lax.rem(me + n - k, n)
            for t in range(len(own)):
                copy = pltpu.make_async_remote_copy(
                    src_ref=own[t],
                    dst_ref=others[t].at[k - 1],
                    send_sem=send_sem.at[k - 1, t],
                    recv_sem=recv_sem.at[k - 1, t],
                    device_id={axis: peer},
                    device_id_type=pl.DeviceIdType.MESH,
                )
                copy.start()
                copies.append(copy)

    components = wpos.shape[0]
    for source, base in ((wpos, 0), (wvel, components)):
        for c in range(components):
            for r in range(water_rows):
                water_s[base + c, pl.ds(r, 1), :] = source[
                    pl.ds(c, 1), pl.ds(r * LANES, LANES)
                ]
    before = [water_s[c] for c in range(components)]
    speed = [water_s[components + c] for c in range(components)]
    after = [b + time_step * v for b, v in zip(before, speed)]
    settled = settle(before, after)
    for c in range(components):
        water_s[c] = speed[c] + (settled[c] - after[c]) / time_step
    for c in range(components):
        for r in range(water_rows):
            out_w[pl.ds(c, 1), pl.ds(r * LANES, LANES)] = water_s[c, pl.ds(r, 1), :]

    def data(k):
        return own if k == 0 else tuple(ref.at[k - 1] for ref in others)

    def index_bonds(k):
        bonds_k = data(k)[3]
        for r in range(bond_rows):
            first_s[k, pl.ds(r, 1), :] = bonds_k[pl.ds(0, 1), pl.ds(r * LANES, LANES)]
            second_s[k, pl.ds(r, 1), :] = bonds_k[pl.ds(1, 1), pl.ds(r * LANES, LANES)]

    def index_cross(k):
        blank = jnp.zeros((con_rows - used, LANES), jnp.int32)
        first_s[k, pl.ds(used, con_rows - used), :] = blank
        second_s[k, pl.ds(used, con_rows - used), :] = blank
        first_s[k, pl.ds(bond_rows, halo_rows), :] = data(k)[5][...]
        second_s[k, pl.ds(bond_rows, halo_rows), :] = data((k + 1) % n)[4][...]

    row_iota = lax.broadcasted_iota(jnp.int32, (atom_rows, LANES), 0)
    lane_iota = lax.broadcasted_iota(jnp.int32, (LANES, LANES), 0)
    pure = bond_rows // SUB
    half_source, half_index = [], []
    for k in range(n):
        sources = [(k, r, first_s, k, 1.0) for r in range(used)]
        sources += [(k, r, second_s, k, -1.0) for r in range(bond_rows)]
        back = (k + n - 1) % n
        sources += [(back, r, second_s, back, -1.0) for r in range(bond_rows, used)]
        sources.sort(key=lambda item: item[1] >= pure * SUB)
        half_source.append([(s[0], s[1]) for s in sources])
        half_index.append(sources)

    def one_hots(k, chosen):
        for p in chosen:
            _, r, ref, slot, sign = half_index[k][p]
            index = ref[slot, pl.ds(r, 1), :]
            rows_s[k, p] = jnp.where(row_iota == (index >> 7), sign, 0.0).astype(
                jnp.bfloat16
            )
            lanes_s[k, :, pl.ds(p * LANES, LANES)] = jnp.where(
                lane_iota == (index & 127), 1.0, 0.0
            ).astype(jnp.bfloat16)

    position = lax.broadcasted_iota(jnp.int32, (SUB, LANES), 0)
    valid = [position + v * SUB < used for v in range(tiles)]

    def one_end(k, v, ref, tables):
        following = (k + 1) % n
        index = ref[k, pl.ds(v * SUB, SUB), :]
        lane, row = index & 127, index >> 7
        low, high = v * SUB, (v + 1) * SUB
        found = [None] * len(tables)
        for r in range(atom_rows):
            hit = row == r
            for c, table in enumerate(tables):
                source = jnp.broadcast_to(table(k, r), (SUB, LANES))
                if ref is second_s and high > bond_rows:
                    there = jnp.broadcast_to(table(following, r), (SUB, LANES))
                    if low < bond_rows:
                        there = jnp.where(position + low < bond_rows, source, there)
                    source = there
                got = lane_gather(source, lane)
                found[c] = got if r == 0 else jnp.where(hit, got, found[c])
        return found

    unit, length, scale, gap, value = (
        [[None] * tiles for _ in range(n)] for _ in range(5)
    )
    tables = []
    for which in (0, 1):
        for c in range(3):
            tables.append(
                lambda slot, r, which=which, c=c: data(slot)[which][
                    pl.ds(c, 1), pl.ds(r * LANES, LANES)
                ]
            )
    tables.append(lambda slot, r: data(slot)[2][pl.ds(r, 1), :])

    def start(k, v):
        at_i = one_end(k, v, first_s, tables)
        at_j = one_end(k, v, second_s, tables)
        diff = minus(at_i[0:3], at_j[0:3])
        size = jnp.where(valid[v], jnp.sqrt(inner(diff, diff)), 1.0)
        moved_i = [p + time_step * q for p, q in zip(at_i[0:3], at_i[3:6])]
        moved_j = [p + time_step * q for p, q in zip(at_j[0:3], at_j[3:6])]
        unit[k][v] = [d / size for d in diff]
        length[k][v] = size
        scale[k][v] = jnp.where(valid[v], 1.0 / jnp.sqrt(at_i[6] + at_j[6]), 0.0)
        gap[k][v] = minus(moved_i, moved_j)
        value[k][v] = scale[k][v] * (inner(unit[k][v], gap[k][v]) - size)

    early = 2 * pure * SUB
    index_bonds(0)
    one_hots(0, range(early))
    for v in range(pure):
        start(0, v)
    for copy in copies:
        copy.wait()
    for k in range(1, n):
        index_bonds(k)
    for k in range(n):
        index_cross(k)
    one_hots(0, range(early, half_rows))
    for k in range(1, n):
        one_hots(k, range(half_rows))
    for k in range(n):
        for v in range(tiles):
            if k > 0 or v >= pure:
                start(k, v)
    scaled_unit = [
        [[scale[k][v] * u for u in unit[k][v]] for v in range(tiles)] for k in range(n)
    ]

    def pack(values, pairs):
        for k, v in pairs:
            rows = pl.ds(v * SUB, SUB)
            for c in range(3):
                weighted = scaled_unit[k][v][c] * values[k][v]
                high = weighted.astype(jnp.bfloat16).astype(jnp.float32)
                packed_s[k, c, rows, :] = high
                packed_s[k, 3 + c, rows, :] = weighted - high

    cuts = []
    for low, high in ((0, early), (early, half_rows)):
        middle = low + (high - low) // 4 * 2
        cuts += [(a, b) for a, b in ((low, middle), (middle, high)) if b > a]

    def make_field(k):
        summed = None
        for low, high in cuts:
            for p in range(low, high):
                slot, r = half_source[k][p]
                hot = rows_s[k, p]
                for j in range(6):
                    wide = jnp.broadcast_to(
                        packed_s[slot, j, pl.ds(r, 1), :], (atom_rows, LANES)
                    ).astype(jnp.bfloat16)
                    lhs_s[k, pl.ds(j * atom_rows, atom_rows), pl.ds(p * LANES, LANES)] = (
                        wide * hot
                    )
            columns = pl.ds(low * LANES, (high - low) * LANES)
            part = lax.dot_general(
                lhs_s[k, :, columns], lanes_s[k, :, columns], (((1,), (1,)), ((), ())),
                preferred_element_type=jnp.float32,
            )
            summed = part if summed is None else summed + part
        weight = data(k)[2][...]
        for c in range(3):
            field_s[k, c] = weight * (
                summed[c * atom_rows:(c + 1) * atom_rows]
                + summed[(3 + c) * atom_rows:(4 + c) * atom_rows]
            )

    field_tables = [
        lambda slot, r, c=c: field_s[slot, c, pl.ds(r, 1), :] for c in range(3)
    ]
    mine = [(0, v) for v in range(tiles)]
    theirs = [(k, v) for k in range(1, n) for v in range(tiles)]
    order = (
        [(0, v) for v in range(pure)]
        + [(k, v) for k in range(n) for v in range(pure, tiles)]
        + [(k, v) for k in range(1, n) for v in range(pure)]
    )

    def other_fields():
        for k in range(1, n):
            make_field(k)

    def field_gaps():
        gaps = [[None] * tiles for _ in range(n)]
        for k, v in order:
            at_i = one_end(k, v, first_s, field_tables)
            at_j = one_end(k, v, second_s, field_tables)
            gaps[k][v] = minus(at_i, at_j)
        return gaps

    def over(function, *series):
        return [
            [function(*[x[k][v] for x in series]) for v in range(tiles)]
            for k in range(n)
        ]

    def one_order(step, carry):
        current, total = carry
        other_fields()
        current = over(
            lambda x, su, g: x - inner(su, g), current, scaled_unit, field_gaps()
        )
        total = over(lambda t, x: t + x, total, current)
        following = over(lambda x, t: jnp.where(step == ORDER - 1, t, x), current, total)
        pack(following, mine + theirs)
        make_field(0)
        return current, total

    def expand(values):
        pack(values, mine + theirs)
        make_field(0)
        lax.fori_loop(0, ORDER, one_order, (values, values))
        return [field_s[0, c] for c in range(3)]

    def one_round(_, carry):
        gap, value, moved_by = carry
        own_field = expand(value)
        other_fields()
        gap = over(minus, gap, field_gaps())
        value = over(
            lambda s, l, g: s * (l - jnp.sqrt(2.0 * l * l - inner(g, g))),
            scale, length, gap,
        )
        return gap, value, [m + f for m, f in zip(moved_by, own_field)]

    zero = jnp.zeros((atom_rows, LANES), jnp.float32)
    gap, value, moved_by = lax.fori_loop(0, ITER, one_round, (gap, value, [zero] * 3))
    moved_by = [m + f for m, f in zip(moved_by, expand(value))]
    for c in range(3):
        field_s[0, c] = moved_by[c] / time_step
    for c in range(3):
        for r in range(atom_rows):
            cols = pl.ds(r * LANES, LANES)
            out_p[pl.ds(c, 1), cols] = (
                vel[pl.ds(c, 1), cols] - field_s[0, c, pl.ds(r, 1), :]
            )


def on_device(
    n, protein_pos, protein_vel, inv_mass, bond_atoms, left_atoms, right_atoms, water_pos, water_vel
):
    atoms = protein_pos.shape[1]
    atom_rows = atoms // LANES
    bond_rows = bond_atoms.shape[1] // LANES
    halo_rows = left_atoms.shape[0] // LANES
    con_rows = -(-(bond_rows + halo_rows + 1) // SUB) * SUB
    half = 2 * (bond_rows + halo_rows)
    others = max(n - 1, 1)
    mass = inv_mass.reshape(atom_rows, LANES)
    left = left_atoms.reshape(halo_rows, LANES)
    right = right_atoms.reshape(halo_rows, LANES)
    operands = (protein_pos, protein_vel, mass, bond_atoms, left, right, water_pos, water_vel)
    vmem = pl.BlockSpec(memory_space=pltpu.VMEM)
    return pl.pallas_call(
        functools.partial(kernel, n, "dom"),
        out_shape=(
            jax.ShapeDtypeStruct(protein_vel.shape, jnp.float32),
            jax.ShapeDtypeStruct(water_vel.shape, jnp.float32),
        ),
        in_specs=[vmem] * len(operands),
        out_specs=(vmem, vmem),
        scratch_shapes=[
            pltpu.VMEM((others,) + x.shape, x.dtype) for x in operands[:6]
        ] + [
            pltpu.VMEM((n, con_rows, LANES), jnp.int32),
            pltpu.VMEM((n, con_rows, LANES), jnp.int32),
            pltpu.VMEM((n, 6, con_rows, LANES), jnp.float32),
            pltpu.VMEM((n, half, atom_rows, LANES), jnp.bfloat16),
            pltpu.VMEM((n, LANES, half * LANES), jnp.bfloat16),
            pltpu.VMEM((n, 6 * atom_rows, half * LANES), jnp.bfloat16),
            pltpu.VMEM((n, 3, atom_rows, LANES), jnp.float32),
            pltpu.VMEM((2 * water_pos.shape[0], water_pos.shape[1] // LANES, LANES), jnp.float32),
            pltpu.SemaphoreType.DMA((others, 6)),
            pltpu.SemaphoreType.DMA((others, 6)),
        ],
        compiler_params=pltpu.CompilerParams(
            collective_id=0, has_side_effects=True, vmem_limit_bytes=60 * 1024 * 1024
        ),
    )(*operands)


def solution(mesh):
    in_specs = (
        P(None, ("rep", "dom")),
        P(None, ("rep", "dom")),
        P(("rep", "dom")),
        P(None, ("rep", "dom")),
        P(("rep", "dom")),
        P(("rep", "dom")),
        P(None, ("rep", "dom")),
        P(None, ("rep", "dom")),
    )
    out_specs = (P(None, ("rep", "dom")), P(None, ("rep", "dom")))
    return jax.shard_map(
        functools.partial(on_device, mesh.shape["dom"]),
        mesh=mesh, in_specs=in_specs, out_specs=out_specs, check_vma=False,
    )
```
